32 devices in a mesh: seq: 8 (over z, y), tp: 4 (over x, core).
Axes of the slice: x: 2, y: 2, z: 4, core: 2. Of those that a mesh axis runs over, the one named last changes fastest.
Arguments:
- tokens: bfloat16 [4096, 2048], P('seq'), may hold values from -16 to 16
- forget: float32 [4096, 32], P('seq', 'tp'), may hold values from -5 to 0, as said below
- attn_gain: float32 [2048], replicated, may hold values from 0.1 to 1.9
- projections: bfloat16 [3, 2048, 2048], P(None, None, 'tp'), may hold values from -0.125 to 0.125
- out_weight: bfloat16 [2048, 2048], P('tp'), may hold values from -0.125 to 0.125
- ffn_gain: float32 [2048], replicated, may hold values from 0.1 to 1.9
- expand_weight: bfloat16 [2, 2048, 4096], P(None, None, 'tp'), may hold values from -0.125 to 0.125
- down_weight: bfloat16 [4096, 2048], P('tp'), may hold values from -0.09375 to 0.09375
Outputs:
- output: bfloat16 [4096, 2048], P('seq')
The draws below stay inside these ranges and needn't reach their ends.
Inputs may be any that keep to these rules, and one draw needn't show every extreme that they name: forget is never positive.
All inputs are finite; a program needn't handle non-finite values.
Results may differ from the reference program's by a relative error of at most 0.011.
Values may be sent and summed in bfloat16 or wider, within the bound.
A program may use at most 128 MiB of HBM per device.

```python
import math
import jax
import jax.numpy as jnp
from jax import lax

D = 2048
HEAD_TOTAL = 32
DH = 64
FF = 4096
TOK_DEV = 512
SEQUENCE_TOKENS = 4096


def draw_tokens(key, part):
    random_keys = jax.random.split(key, 3)
    noise = jax.random.normal(random_keys[0], (SEQUENCE_TOKENS, D), jnp.float32)
    row_scale = jnp.exp(jax.random.uniform(random_keys[1], (SEQUENCE_TOKENS, 1), jnp.float32, jnp.log(0.3), jnp.log(3.0)))
    column_scale = jnp.exp(jax.random.uniform(random_keys[2], (1, D), jnp.float32, jnp.log(0.3), jnp.log(3.0)))
    return jnp.clip(noise * row_scale * column_scale, -16.0, 16.0).astype(jnp.bfloat16)


def draw_forget(key, part):
    random_keys = jax.random.split(key, 7)
    slow_share = 0.5
    is_slow = jax.random.uniform(random_keys[0], (HEAD_TOTAL,), jnp.float32) < slow_share
    slow_rate = jax.random.uniform(random_keys[1], (HEAD_TOTAL,), jnp.float32, 0.2, 0.6) / SEQUENCE_TOKENS
    fast_rate = jnp.exp(jax.random.uniform(random_keys[2], (HEAD_TOTAL,), jnp.float32, jnp.log(10.0), jnp.log(16.0))) / TOK_DEV
    base_rate = jnp.where(is_slow, slow_rate, fast_rate)
    block_count = SEQUENCE_TOKENS // TOK_DEV
    device_factor = jnp.exp(jax.random.uniform(random_keys[3], (block_count, 1, HEAD_TOTAL), jnp.float32, jnp.log(0.5), jnp.log(2.0)))
    roughness = jax.random.uniform(random_keys[4], (block_count, TOK_DEV, HEAD_TOTAL), jnp.float32, 0.5, 1.5)
    decay_rates = (base_rate * device_factor * roughness).reshape(SEQUENCE_TOKENS, HEAD_TOTAL)
    spike_positions = jax.random.randint(random_keys[5], (2,), 0, SEQUENCE_TOKENS)
    spike_magnitude = jax.random.uniform(random_keys[6], (2, HEAD_TOTAL), jnp.float32, 0.22, 0.69)
    spike_flags = (jnp.arange(SEQUENCE_TOKENS)[:, None] == spike_positions[None, :]).astype(jnp.float32)
    spike_values = jnp.dot(spike_flags, spike_magnitude)
    return -(decay_rates + spike_values)


def block_scale(key, extent, shards, least, top_value):
    factor_of, own = 1.0, jax.random.fold_in(key, 6)
    for axis_at, blocks in shards:
        draws = jnp.exp(jax.random.uniform(jax.random.fold_in(own, axis_at), (blocks,), jnp.float32, least / len(shards), top_value / len(shards)))
        factor_of = factor_of * jnp.repeat(draws, extent[axis_at] // blocks).reshape([-1 if axis == axis_at else 1 for axis in range(len(extent))])
    return factor_of


def gaussian(stream_key, shape, width, reach, shards=(), dtype=jnp.bfloat16):
    entries = width * jax.random.normal(stream_key, shape, jnp.float32)
    if shards:
        entries = entries * block_scale(stream_key, shape, shards, -0.22, 0.18)
    return jnp.clip(entries, -reach, reach).astype(dtype)


def setup_inputs(seed: int = 0) -> dict:
    splits = jax.random.split(jax.random.key(seed), 9)
    tokens = draw_tokens(jax.random.fold_in(splits[8], 71), 0)
    forget = draw_forget(jax.random.fold_in(splits[8], 71), 0)
    attn_gain = jnp.clip(1.0 + 0.18 * jax.random.normal(splits[2], (D,), jnp.float32), 0.1, 1.9)
    projections = gaussian(splits[3], (3, D, HEAD_TOTAL * DH), D ** -0.5, 0.125, ((2, 4),))
    out_weight = gaussian(splits[4], (HEAD_TOTAL * DH, D), (HEAD_TOTAL * DH) ** -0.5, 0.125, ((0, 4),))
    ffn_gain = jnp.clip(1.0 + 0.18 * jax.random.normal(splits[5], (D,), jnp.float32), 0.1, 1.9)
    expand_weight = gaussian(splits[6], (2, D, FF), D ** -0.5, 0.125, ((2, 4),))
    down_weight = gaussian(splits[7], (FF, D), FF ** -0.5, 0.09375, ((0, 4),))
    return dict(tokens=tokens, forget=forget, attn_gain=attn_gain, projections=projections, out_weight=out_weight, ffn_gain=ffn_gain, expand_weight=expand_weight, down_weight=down_weight)


norm_epsilon = 1e-05
head_epsilon = 1e-06

def rms_scale(values, gain_vector):
    widened = values.astype(jnp.float32)
    mean_square = lax.optimization_barrier(jnp.mean(widened * widened, axis=-1, keepdims=True))
    return widened * lax.rsqrt(mean_square + norm_epsilon) * gain_vector

def summarize(key_rows, value_rows, forget_rows):
    log_decay = jnp.cumsum(forget_rows, axis=0)
    block_total = log_decay[-1]
    shrink_factors = jnp.exp(block_total[None, :] - log_decay)
    scaled_keys = (key_rows.astype(jnp.float32) * shrink_factors[:, :, None]).astype(jnp.bfloat16)
    block_state = jnp.einsum('shd,she->hde', scaled_keys.astype(jnp.float32), value_rows.astype(jnp.float32), precision=lax.Precision.HIGHEST)
    return (log_decay, block_total, block_state)

def attend_local(query_rows, key_rows, value_rows, log_decay, incoming):
    head_size = query_rows.shape[2]
    score_scale = 1.0 / math.sqrt(head_size)
    query_wide = query_rows.astype(jnp.float32)
    scores = jnp.einsum('thd,shd->hts', query_wide, key_rows.astype(jnp.float32), precision=lax.Precision.HIGHEST) * score_scale
    log_gaps = log_decay.T[:, :, None] - log_decay.T[:, None, :]
    row_order = jnp.arange(query_rows.shape[0])
    causal = (row_order[:, None] >= row_order[None, :])[None]
    local_weights = jnp.where(causal, scores * jnp.exp(jnp.where(causal, log_gaps, 0.0)), 0.0).astype(jnp.bfloat16)
    local_part = jnp.einsum('hts,she->the', local_weights.astype(jnp.float32), value_rows.astype(jnp.float32), precision=lax.Precision.HIGHEST)
    carried = jnp.einsum('thd,hde->the', query_wide, incoming, precision=lax.Precision.HIGHEST)
    attended = local_part + carried * (jnp.exp(log_decay) * score_scale)[:, :, None]
    mean_square = lax.optimization_barrier(jnp.mean(attended * attended, axis=-1, keepdims=True))
    return (attended * lax.rsqrt(mean_square + head_epsilon)).astype(jnp.bfloat16)

def reference(tokens, forget, attn_gain, projections, out_weight, ffn_gain, expand_weight, down_weight):
    normed = rms_scale(tokens, attn_gain).astype(jnp.bfloat16)
    block_count = SEQUENCE_TOKENS // TOK_DEV
    shaped = []
    for which in range(3):
        projected = jnp.dot(normed, projections[which], preferred_element_type=jnp.float32).astype(jnp.bfloat16)
        shaped.append(projected.reshape(block_count, TOK_DEV, HEAD_TOTAL, DH))
    forget_blocks = forget.reshape(block_count, TOK_DEV, HEAD_TOTAL)

    def block_step(incoming, block_data):
        query_rows, key_rows, value_rows, forget_rows = block_data
        log_decay, block_total, block_state = summarize(key_rows, value_rows, forget_rows)
        head_out = attend_local(query_rows, key_rows, value_rows, log_decay, incoming)
        following = jnp.exp(block_total)[:, None, None] * incoming + block_state
        return (following, head_out)
    start_state = jnp.zeros((HEAD_TOTAL, DH, DH), jnp.float32)
    _, head_blocks = lax.scan(block_step, start_state, (shaped[0], shaped[1], shaped[2], forget_blocks))
    head_out = head_blocks.reshape(SEQUENCE_TOKENS, HEAD_TOTAL * DH)
    attn_out = jnp.dot(head_out, out_weight, preferred_element_type=jnp.float32)
    residual = (tokens.astype(jnp.float32) + attn_out).astype(jnp.bfloat16)
    normed_ffn = rms_scale(residual, ffn_gain).astype(jnp.bfloat16)
    gate_proj = jnp.dot(normed_ffn, expand_weight[0], preferred_element_type=jnp.float32)
    up_proj = jnp.dot(normed_ffn, expand_weight[1], preferred_element_type=jnp.float32)
    hidden = (jax.nn.silu(gate_proj) * up_proj).astype(jnp.bfloat16)
    ffn_out = jnp.dot(hidden, down_weight, preferred_element_type=jnp.float32)
    return (residual.astype(jnp.float32) + ffn_out).astype(jnp.bfloat16)
```

```python
import functools

import jax
import jax.numpy as jnp
from jax import lax
from jax.experimental import pallas as pl
from jax.experimental.pallas import tpu as pltpu
from jax.sharding import PartitionSpec as P

norm_epsilon = 1e-05
head_epsilon = 1e-06
MESH = pl.DeviceIdType.MESH
CHUNKS = 4
F32 = jnp.float32
BF16 = jnp.bfloat16


def dot(a, b):
    return jnp.dot(a, b, preferred_element_type=F32)


def contract(a, b, dim_a, dim_b):
    return lax.dot_general(
        a, b, (((dim_a,), (dim_b,)), ((), ())), preferred_element_type=F32
    )


def normalize(widened, gain):
    mean_square = jnp.mean(widened * widened, axis=-1, keepdims=True)
    return (widened * lax.rsqrt(mean_square + norm_epsilon) * gain).astype(BF16)


def kernel(
    blocks, steps,
    tok_hbm, fg, fgt, again, proj_hbm, ow_hbm, fgain, ew_hbm, dw_hbm,
    out_hbm,
    tok, wq, wk, wv, wo, wg, wu, wd,
    normed, q, k, v, att, ho, bd, es, el, ts, tl, tsb, tsl, trb, trl,
    part, own, dsend1, drecv1, xsend1, xrecv1, nf, res, hid,
    dsend2, drecv2, xsend2, xrecv2, outb,
    ld, ldt,
    wsem, sts, strv, d1s, d1r, x1s, x1r, ns, nr, d2s, d2r, x2s, x2r, osd, orv, olc,
):
    rows, width = tok.shape
    heads = fg.shape[1]
    pairs = heads // 2
    chunk = rows // CHUNKS
    half = chunk // 2
    me = lax.axis_index("seq")
    tp = lax.axis_index("tp")
    core = lax.rem(tp, 2)
    partner = tp + 1 - 2 * core
    across = lax.rem(tp + 2, 4)

    loads = []
    for at, (src, dst) in enumerate((
        (tok_hbm, tok), (proj_hbm.at[1], wk), (proj_hbm.at[2], wv), (proj_hbm.at[0], wq),
        (ow_hbm, wo), (ew_hbm.at[0], wg), (ew_hbm.at[1], wu), (dw_hbm, wd),
    )):
        copy = pltpu.make_async_copy(src, dst, wsem.at[at])
        copy.start()
        loads.append(copy)

    barrier = pltpu.get_barrier_semaphore()
    for other in (partner, across):
        pl.semaphore_signal(barrier, inc=1, device_id={"tp": other}, device_id_type=MESH)
    for step in range(steps):
        for far in (2 ** step, blocks - 2 ** step):
            pl.semaphore_signal(
                barrier, inc=1, device_id={"seq": lax.rem(me + far, blocks)}, device_id_type=MESH)

    tri = (
        lax.broadcasted_iota(jnp.int32, (rows, rows), 0)
        >= lax.broadcasted_iota(jnp.int32, (rows, rows), 1)
    ).astype(F32)
    ld[...] = lax.dot_general(
        tri, fg[...], (((1,), (0,)), ((), ())),
        precision=lax.Precision.HIGHEST, preferred_element_type=F32,
    )
    ldt[...] = lax.dot_general(
        fgt[...], tri, (((1,), (1,)), ((), ())),
        precision=lax.Precision.HIGHEST, preferred_element_type=F32,
    )

    loads[0].wait()

    def norm_chunk(r, carry):
        at = pl.ds(pl.multiple_of(r * chunk, chunk), chunk)
        normed[at, :] = normalize(tok[at, :].astype(F32), again[...])
        return carry

    lax.fori_loop(0, CHUNKS, norm_chunk, 0)

    def project(weight, dst):
        tile = min(256, dst.shape[1])

        def body(j, carry):
            at = pl.ds(pl.multiple_of(j * tile, tile), tile)
            dst[:, at] = dot(normed[...], weight[:, at]).astype(BF16)
            return carry

        lax.fori_loop(0, dst.shape[1] // tile, body, 0)

    loads[1].wait()
    project(wk, k)
    loads[2].wait()
    project(wv, v)

    low = lax.broadcasted_iota(jnp.int32, (1, 128), 1) < 64
    low_f = low.astype(F32)
    masks_f = (low_f, 1.0 - low_f)
    masks = (masks_f[0].astype(BF16), masks_f[1].astype(BF16))

    def spread(columns, p):
        return jnp.where(low, columns[:, 2 * p : 2 * p + 1], columns[:, 2 * p + 1 : 2 * p + 2])

    log_decay = ld[...]
    last = log_decay[rows - 1 : rows, :]
    shrink = jnp.exp(last - log_decay)
    tl[...] = jnp.zeros_like(tl)
    el[...] = jnp.zeros_like(el)
    es[...] = jnp.zeros_like(es)
    for p in range(pairs):
        lanes = slice(128 * p, 128 * p + 128)
        scaled = (k[:, lanes].astype(F32) * spread(shrink, p)).astype(BF16)
        state = contract(scaled, v[:, lanes], 0, 0)
        ts[64 * p : 64 * p + 64, :] = state[:64] * masks_f[0] + state[64:] * masks_f[1]
        tl[p : p + 1, :] = spread(last, p)

    pl.semaphore_wait(barrier, 2 + 2 * steps)

    def state_copies(step):
        far = 2 ** step
        return (
            pltpu.make_async_remote_copy(
                tsb.at[step], trb.at[step], sts.at[step, 0], strv.at[step, 0],
                device_id={"seq": me + far}, device_id_type=MESH),
            pltpu.make_async_remote_copy(
                tsl.at[step], trl.at[step], sts.at[step, 1], strv.at[step, 1],
                device_id={"seq": me + far}, device_id_type=MESH),
        )

    def send_state(step):
        @pl.when(me + 2 ** step < blocks)
        def _():
            tsb[step] = ts[...].astype(BF16)
            tsl[step] = tl[...]
            for copy in state_copies(step):
                copy.start()

    def take_state(step):
        @pl.when(me >= 2 ** step)
        def _():
            for copy in state_copies(step):
                copy.wait_recv()
            e_decay = jnp.exp(el[...])
            t_decay = jnp.exp(tl[...])
            for p in range(pairs):
                at = slice(64 * p, 64 * p + 64)
                came = trb[step, at, :].astype(F32)
                es[at, :] = es[at, :] + e_decay[p : p + 1, :] * came
                ts[at, :] = ts[at, :] + t_decay[p : p + 1, :] * came
            el[...] = el[...] + trl[step]
            tl[...] = tl[...] + trl[step]

        if step + 1 < steps:
            send_state(step + 1)

    if steps:
        send_state(0)
    loads[3].wait()
    project(wq, q)

    span = rows // 2
    taken = 0
    for p in range(pairs):
        lanes = slice(128 * p, 128 * p + 128)
        for piece in range(2):
            at = slice(piece * span, piece * span + span)
            reach = (piece + 1) * span
            causal = (
                lax.broadcasted_iota(jnp.int32, (span, reach), 0) + piece * span
                >= lax.broadcasted_iota(jnp.int32, (span, reach), 1)
            )
            sums = []
            for j in range(2):
                h = 2 * p + j
                scores = contract(q[at, lanes] * masks[j], k[:reach, lanes], 1, 1)
                gaps = jnp.where(causal, ld[at, h : h + 1] - ldt[h : h + 1, :reach], -1e30)
                weights = (scores * 0.125 * jnp.exp(gaps)).astype(BF16)
                sums.append(dot(weights, v[:reach, lanes]))
            att[at, lanes] = jnp.where(low, sums[0], sums[1])
        if taken < steps:
            take_state(taken)
            taken += 1
    while taken < steps:
        take_state(taken)
        taken += 1

    for p in range(pairs):
        came = es[64 * p : 64 * p + 64, :]
        bd[p] = jnp.concatenate([came * masks_f[0], came * masks_f[1]], axis=0).astype(BF16)
    same_head = (
        (lax.broadcasted_iota(jnp.int32, (128, 128), 0) < 64)
        == (lax.broadcasted_iota(jnp.int32, (128, 128), 1) < 64)
    ).astype(F32).astype(BF16)

    def whole_rows(r):
        return pl.ds(pl.multiple_of(r * chunk, chunk), chunk)

    def own_rows(r):
        return pl.ds(pl.multiple_of(r * chunk + core * half, half), half)

    mine = pl.ds(pl.multiple_of(core * half, half), half)
    theirs = pl.ds(pl.multiple_of(half - core * half, half), half)

    def to(src, dst, ssem, rsem, other):
        return pltpu.make_async_remote_copy(
            src, dst, ssem, rsem, device_id={"tp": other}, device_id_type=MESH)

    def d1(r):
        return to(dsend1.at[r], drecv1.at[r], d1s.at[r], d1r.at[r], partner)

    def x1(r):
        return to(xsend1.at[r], xrecv1.at[r], x1s.at[r], x1r.at[r], across)

    def nfc(r):
        return to(nf.at[own_rows(r)], nf.at[own_rows(r)], ns.at[r], nr.at[r], partner)

    def d2(r):
        return to(dsend2.at[r], drecv2.at[r], d2s.at[r], d2r.at[r], partner)

    def x2(r):
        return to(xsend2.at[r], xrecv2.at[r], x2s.at[r], x2r.at[r], across)

    def oc(r):
        return to(outb.at[r], out_hbm.at[own_rows(r)], osd.at[r], orv.at[r], partner)

    def ol(r):
        return pltpu.make_async_copy(outb.at[r], out_hbm.at[own_rows(r)], olc.at[r])

    loads[4].wait()
    wide = min(512, width)

    def attend(r, carry):
        at = whole_rows(r)
        reach_decay = jnp.exp(ld[at, :]) * 0.125
        for p in range(pairs):
            lanes = slice(128 * p, 128 * p + 128)
            attended = att[at, lanes] + dot(q[at, lanes], bd[p]) * spread(reach_decay, p)
            mean_square = dot((attended * attended).astype(BF16), same_head) * (1.0 / 64)
            ho[at, lanes] = (attended * lax.rsqrt(mean_square + head_epsilon)).astype(BF16)
        for c in range(width // wide):
            cols = slice(c * wide, c * wide + wide)
            part[:, cols] = dot(ho[at, :], wo[:, cols])
        own[r] = part[mine, :]
        dsend1[r] = part[theirs, :].astype(BF16)
        d1(r).start()
        return carry

    def cross1(r):
        d1(r).wait_recv()
        xsend1[r] = (own[r] + drecv1[r].astype(F32)).astype(BF16)
        x1(r).start()

    def attend_cross(r, carry):
        attend(r, 0)

        @pl.when(r > 0)
        def _():
            cross1(r - 1)

        return carry

    lax.fori_loop(0, CHUNKS, attend_cross, 0)
    cross1(CHUNKS - 1)
    for at in (5, 6, 7):
        loads[at].wait()

    hidden_width = wg.shape[1]
    tile = min(256, hidden_width)

    def forward(r, carry):
        x1(r).wait_recv()
        added = xsend1[r].astype(F32) + xrecv1[r].astype(F32)
        kept = (tok[own_rows(r), :].astype(F32) + added).astype(BF16)
        res[r] = kept
        nf[own_rows(r), :] = normalize(kept.astype(F32), fgain[...])
        nfc(r).start()
        nfc(r).wait_recv()
        at = whole_rows(r)
        for c in range(hidden_width // tile):
            cols = slice(c * tile, c * tile + tile)
            gate = dot(nf[at, :], wg[:, cols])
            up = dot(nf[at, :], wu[:, cols])
            hid[:, cols] = (gate / (1.0 + jnp.exp(-gate)) * up).astype(BF16)
        for c in range(width // wide):
            cols = slice(c * wide, c * wide + wide)
            part[:, cols] = dot(hid[...], wd[:, cols])
        own[r] = part[mine, :]
        dsend2[r] = part[theirs, :].astype(BF16)
        d2(r).start()
        d2(r).wait_recv()
        xsend2[r] = (own[r] + drecv2[r].astype(F32)).astype(BF16)
        x2(r).start()
        return carry

    lax.fori_loop(0, CHUNKS, forward, 0)

    def finish(r, carry):
        x2(r).wait_recv()
        added = xsend2[r].astype(F32) + xrecv2[r].astype(F32)
        outb[r] = (res[r].astype(F32) + added).astype(BF16)
        oc(r).start()
        ol(r).start()
        return carry

    lax.fori_loop(0, CHUNKS, finish, 0)

    def drain(r, carry):
        for copy in (d1(r), x1(r), nfc(r), d2(r), x2(r)):
            copy.wait_send()
        oc(r).wait()
        ol(r).wait()
        return carry

    lax.fori_loop(0, CHUNKS, drain, 0)
    for step in range(steps):
        @pl.when(me + 2 ** step < blocks)
        def _():
            for copy in state_copies(step):
                copy.wait_send()


def local(blocks, tokens, forget, attn_gain, projections, out_weight, ffn_gain, expand_weight, down_weight):
    rows, width = tokens.shape
    heads = forget.shape[1]
    inner = projections.shape[2]
    hidden = down_weight.shape[0]
    pairs = heads // 2
    steps = max(blocks - 1, 0).bit_length()
    chunk = rows // CHUNKS
    half = chunk // 2
    V = pltpu.VMEM
    S = pltpu.SemaphoreType.DMA
    slots = max(steps, 1)
    piece = V((CHUNKS, half, width), BF16)
    scratch = [
        V((rows, width), BF16),
        V((width, inner), BF16), V((width, inner), BF16), V((width, inner), BF16),
        V((inner, width), BF16),
        V((width, hidden), BF16), V((width, hidden), BF16), V((hidden, width), BF16),
        V((rows, width), BF16),
        V((rows, inner), BF16), V((rows, inner), BF16), V((rows, inner), BF16),
        V((rows, inner), F32), V((rows, inner), BF16),
        V((pairs, 128, 128), BF16),
        V((64 * pairs, 128), F32), V((8, 128), F32), V((64 * pairs, 128), F32), V((8, 128), F32),
        V((slots, 64 * pairs, 128), BF16), V((slots, 8, 128), F32),
        V((slots, 64 * pairs, 128), BF16), V((slots, 8, 128), F32),
        V((chunk, width), F32), V((CHUNKS, half, width), F32),
        piece, piece, piece, piece,
        V((rows, width), BF16), piece, V((chunk, hidden), BF16),
        piece, piece, piece, piece, piece,
        V((rows, heads), F32), V((heads, rows), F32),
        S((8,)), S((slots, 2)), S((slots, 2)),
    ] + [S((CHUNKS,)) for _ in range(13)]
    hbm = pl.BlockSpec(memory_space=pl.ANY)
    vmem = pl.BlockSpec(memory_space=pltpu.VMEM)
    return pl.pallas_call(
        functools.partial(kernel, blocks, steps),
        out_shape=jax.ShapeDtypeStruct((rows, width), BF16),
        in_specs=[hbm, vmem, vmem, vmem, hbm, hbm, vmem, hbm, hbm],
        out_specs=hbm,
        scratch_shapes=scratch,
        compiler_params=pltpu.CompilerParams(
            collective_id=0, has_side_effects=True, vmem_limit_bytes=64_000_000
        ),
    )(
        tokens, forget, forget.T, attn_gain[None, :], projections, out_weight,
        ffn_gain[None, :], expand_weight, down_weight,
    )


def solution(mesh):
    placed = (
        P("seq", None),
        P("seq", "tp"),
        P(),
        P(None, None, "tp"),
        P("tp", None),
        P(),
        P(None, None, "tp"),
        P("tp", None),
    )
    return jax.shard_map(
        functools.partial(local, mesh.shape["seq"]),
        mesh=mesh, in_specs=placed, out_specs=P("seq", None), check_vma=False,
    )
```

```python
import functools

import jax
import jax.numpy as jnp
from jax import lax
from jax.experimental import pallas as pl
from jax.experimental.pallas import tpu as pltpu
from jax.sharding import PartitionSpec as P

norm_epsilon = 1e-05
head_epsilon = 1e-06
MESH = pl.DeviceIdType.MESH
CHUNKS = 4
F32 = jnp.float32
BF16 = jnp.bfloat16


def dot(a, b):
    return jnp.dot(a, b, preferred_element_type=F32)


def contract(a, b, dim_a, dim_b):
    return lax.dot_general(
        a, b, (((dim_a,), (dim_b,)), ((), ())), preferred_element_type=F32
    )


def normalize(widened, gain):
    mean_square = jnp.mean(widened * widened, axis=-1, keepdims=True)
    return (widened * lax.rsqrt(mean_square + norm_epsilon) * gain).astype(BF16)


def kernel(
    blocks, steps,
    tok_hbm, fgt, again, proj_hbm, ow_hbm, fgain, ew_hbm, dw_hbm,
    out_hbm,
    tok, wq, wk, wv, wo, wg, wu, wd,
    normed, q, k, v, att, ho, bd, es, el, ts, tl, tsb, tsl, trb, trl,
    part, own, dsend1, drecv1, xsend1, xrecv1, nf, res, hid,
    dsend2, drecv2, xsend2, xrecv2, outb,
    ld, ldt,
    wsem, sts, strv, d1s, d1r, x1s, x1r, ns, nr, d2s, d2r, x2s, x2r, osd, orv, olc,
):
    rows, width = tok.shape
    heads = fgt.shape[0]
    pairs = heads // 2
    chunk = rows // CHUNKS
    half = chunk // 2
    me = lax.axis_index("seq")
    tp = lax.axis_index("tp")
    core = lax.rem(tp, 2)
    partner = tp + 1 - 2 * core
    across = lax.rem(tp + 2, 4)

    loads = []
    for at, (src, dst) in enumerate((
        (tok_hbm, tok), (proj_hbm.at[1], wk), (proj_hbm.at[2], wv), (proj_hbm.at[0], wq),
        (ow_hbm, wo), (ew_hbm.at[0], wg), (ew_hbm.at[1], wu), (dw_hbm, wd),
    )):
        copy = pltpu.make_async_copy(src, dst, wsem.at[at])
        loads.append(copy)
    for at in range(3):
        loads[at].start()

    barrier = pltpu.get_barrier_semaphore()
    for other in (partner, across):
        pl.semaphore_signal(barrier, inc=1, device_id={"tp": other}, device_id_type=MESH)
    for step in range(steps):
        for far in (2 ** step, blocks - 2 ** step):
            pl.semaphore_signal(
                barrier, inc=1, device_id={"seq": lax.rem(me + far, blocks)}, device_id_type=MESH)

    tri = (
        lax.broadcasted_iota(jnp.int32, (rows, rows), 0)
        >= lax.broadcasted_iota(jnp.int32, (rows, rows), 1)
    ).astype(F32)
    ld[...] = lax.dot_general(
        tri, fgt[...], (((1,), (1,)), ((), ())),
        precision=lax.Precision.HIGHEST, preferred_element_type=F32,
    )
    ldt[...] = lax.dot_general(
        fgt[...], tri, (((1,), (1,)), ((), ())),
        precision=lax.Precision.HIGHEST, preferred_element_type=F32,
    )

    loads[0].wait()
    loads[3].start()
    loads[4].start()

    def norm_chunk(r, carry):
        at = pl.ds(pl.multiple_of(r * chunk, chunk), chunk)
        normed[at, :] = normalize(tok[at, :].astype(F32), again[...])
        return carry

    lax.fori_loop(0, CHUNKS, norm_chunk, 0)

    def project(weight, dst):
        tile = min(256, dst.shape[1])

        def body(j, carry):
            at = pl.ds(pl.multiple_of(j * tile, tile), tile)
            dst[:, at] = dot(normed[...], weight[:, at]).astype(BF16)
            return carry

        lax.fori_loop(0, dst.shape[1] // tile, body, 0)

    loads[1].wait()
    project(wk, k)
    loads[2].wait()
    project(wv, v)

    low = lax.broadcasted_iota(jnp.int32, (1, 128), 1) < 64
    low_f = low.astype(F32)
    masks_f = (low_f, 1.0 - low_f)
    masks = (masks_f[0].astype(BF16), masks_f[1].astype(BF16))

    def spread(columns, p):
        return jnp.where(low, columns[:, 2 * p : 2 * p + 1], columns[:, 2 * p + 1 : 2 * p + 2])

    log_decay = ld[...]
    last = log_decay[rows - 1 : rows, :]
    shrink = jnp.exp(last - log_decay)
    tl[...] = jnp.zeros_like(tl)
    el[...] = jnp.zeros_like(el)
    es[...] = jnp.zeros_like(es)
    for p in range(pairs):
        lanes = slice(128 * p, 128 * p + 128)
        scaled = (k[:, lanes].astype(F32) * spread(shrink, p)).astype(BF16)
        state = contract(scaled, v[:, lanes], 0, 0)
        ts[64 * p : 64 * p + 64, :] = state[:64] * masks_f[0] + state[64:] * masks_f[1]
        tl[p : p + 1, :] = spread(last, p)

    pl.semaphore_wait(barrier, 2 + 2 * steps)

    def state_copies(step):
        far = 2 ** step
        return (
            pltpu.make_async_remote_copy(
                tsb.at[step], trb.at[step], sts.at[step, 0], strv.at[step, 0],
                device_id={"seq": me + far}, device_id_type=MESH),
            pltpu.make_async_remote_copy(
                tsl.at[step], trl.at[step], sts.at[step, 1], strv.at[step, 1],
                device_id={"seq": me + far}, device_id_type=MESH),
        )

    def send_state(step):
        @pl.when(me + 2 ** step < blocks)
        def _():
            tsb[step] = ts[...].astype(BF16)
            tsl[step] = tl[...]
            for copy in state_copies(step):
                copy.start()

    def take_state(step):
        @pl.when(me >= 2 ** step)
        def _():
            for copy in state_copies(step):
                copy.wait_recv()
            e_decay = jnp.exp(el[...])
            t_decay = jnp.exp(tl[...])
            for p in range(pairs):
                at = slice(64 * p, 64 * p + 64)
                came = trb[step, at, :].astype(F32)
                es[at, :] = es[at, :] + e_decay[p : p + 1, :] * came
                ts[at, :] = ts[at, :] + t_decay[p : p + 1, :] * came
            el[...] = el[...] + trl[step]
            tl[...] = tl[...] + trl[step]

        if step + 1 < steps:
            send_state(step + 1)

    if steps:
        send_state(0)
    for at in (5, 6, 7):
        loads[at].start()
    loads[3].wait()
    project(wq, q)

    span = rows // 2
    taken = 0
    for p in range(pairs):
        lanes = slice(128 * p, 128 * p + 128)
        for piece in range(2):
            at = slice(piece * span, piece * span + span)
            reach = (piece + 1) * span
            causal = (
                lax.broadcasted_iota(jnp.int32, (span, reach), 0) + piece * span
                >= lax.broadcasted_iota(jnp.int32, (span, reach), 1)
            )
            sums = []
            for j in range(2):
                h = 2 * p + j
                scores = contract(q[at, lanes] * masks[j], k[:reach, lanes], 1, 1)
                gaps = jnp.where(causal, ld[at, h : h + 1] - ldt[h : h + 1, :reach], -1e30)
                weights = (scores * 0.125 * jnp.exp(gaps)).astype(BF16)
                sums.append(dot(weights, v[:reach, lanes]))
            att[at, lanes] = jnp.where(low, sums[0], sums[1])
        if p % 2 and taken < steps:
            take_state(taken)
            taken += 1
    while taken < steps:
        take_state(taken)
        taken += 1

    for p in range(pairs):
        came = es[64 * p : 64 * p + 64, :]
        bd[p] = jnp.concatenate([came * masks_f[0], came * masks_f[1]], axis=0).astype(BF16)
    same_head = (
        (lax.broadcasted_iota(jnp.int32, (128, 128), 0) < 64)
        == (lax.broadcasted_iota(jnp.int32, (128, 128), 1) < 64)
    ).astype(F32).astype(BF16)

    def whole_rows(r):
        return pl.ds(pl.multiple_of(r * chunk, chunk), chunk)

    def own_rows(r):
        return pl.ds(pl.multiple_of(r * chunk + core * half, half), half)

    mine = pl.ds(pl.multiple_of(core * half, half), half)
    theirs = pl.ds(pl.multiple_of(half - core * half, half), half)

    def to(src, dst, ssem, rsem, other):
        return pltpu.make_async_remote_copy(
            src, dst, ssem, rsem, device_id={"tp": other}, device_id_type=MESH)

    def d1(r):
        return to(dsend1.at[r], drecv1.at[r], d1s.at[r], d1r.at[r], partner)

    def x1(r):
        return to(xsend1.at[r], xrecv1.at[r], x1s.at[r], x1r.at[r], across)

    def nfc(r):
        return to(nf.at[own_rows(r)], nf.at[own_rows(r)], ns.at[r], nr.at[r], partner)

    def d2(r):
        return to(dsend2.at[r], drecv2.at[r], d2s.at[r], d2r.at[r], partner)

    def x2(r):
        return to(xsend2.at[r], xrecv2.at[r], x2s.at[r], x2r.at[r], across)

    def oc(r):
        return to(outb.at[r], out_hbm.at[own_rows(r)], osd.at[r], orv.at[r], partner)

    def ol(r):
        return pltpu.make_async_copy(outb.at[r], out_hbm.at[own_rows(r)], olc.at[r])

    loads[4].wait()
    wide = min(512, width)

    def attend(r, carry):
        at = whole_rows(r)
        reach_decay = jnp.exp(ld[at, :]) * 0.125
        for p in range(pairs):
            lanes = slice(128 * p, 128 * p + 128)
            attended = att[at, lanes] + dot(q[at, lanes], bd[p]) * spread(reach_decay, p)
            mean_square = dot((attended * attended).astype(BF16), same_head) * (1.0 / 64)
            ho[at, lanes] = (attended * lax.rsqrt(mean_square + head_epsilon)).astype(BF16)
        for c in range(width // wide):
            cols = slice(c * wide, c * wide + wide)
            part[:, cols] = dot(ho[at, :], wo[:, cols])
        own[r] = part[mine, :]
        dsend1[r] = part[theirs, :].astype(BF16)
        d1(r).start()
        return carry

    def cross1(r):
        d1(r).wait_recv()
        xsend1[r] = (own[r] + drecv1[r].astype(F32)).astype(BF16)
        x1(r).start()

    def attend_cross(r, carry):
        attend(r, 0)

        @pl.when(r > 0)
        def _():
            cross1(r - 1)

        return carry

    lax.fori_loop(0, CHUNKS, attend_cross, 0)
    cross1(CHUNKS - 1)
    for at in (5, 6, 7):
        loads[at].wait()

    hidden_width = wg.shape[1]
    tile = min(256, hidden_width)

    def forward(r, carry):
        x1(r).wait_recv()
        added = xsend1[r].astype(F32) + xrecv1[r].astype(F32)
        kept = (tok[own_rows(r), :].astype(F32) + added).astype(BF16)
        res[r] = kept
        nf[own_rows(r), :] = normalize(kept.astype(F32), fgain[...])
        nfc(r).start()
        nfc(r).wait_recv()
        at = whole_rows(r)
        for c in range(hidden_width // tile):
            cols = slice(c * tile, c * tile + tile)
            gate = dot(nf[at, :], wg[:, cols])
            up = dot(nf[at, :], wu[:, cols])
            hid[:, cols] = (gate / (1.0 + jnp.exp(-gate)) * up).astype(BF16)
        for c in range(width // wide):
            cols = slice(c * wide, c * wide + wide)
            part[:, cols] = dot(hid[...], wd[:, cols])
        own[r] = part[mine, :]
        dsend2[r] = part[theirs, :].astype(BF16)
        d2(r).start()
        d2(r).wait_recv()
        xsend2[r] = (own[r] + drecv2[r].astype(F32)).astype(BF16)
        x2(r).start()
        return carry

    lax.fori_loop(0, CHUNKS, forward, 0)

    def finish(r, carry):
        x2(r).wait_recv()
        added = xsend2[r].astype(F32) + xrecv2[r].astype(F32)
        outb[r] = (res[r].astype(F32) + added).astype(BF16)
        oc(r).start()
        ol(r).start()
        return carry

    lax.fori_loop(0, CHUNKS, finish, 0)

    def drain(r, carry):
        for copy in (d1(r), x1(r), nfc(r), d2(r), x2(r)):
            copy.wait_send()
        oc(r).wait()
        ol(r).wait()
        return carry

    lax.fori_loop(0, CHUNKS, drain, 0)
    for step in range(steps):
        @pl.when(me + 2 ** step < blocks)
        def _():
            for copy in state_copies(step):
                copy.wait_send()


def local(blocks, tokens, forget, attn_gain, projections, out_weight, ffn_gain, expand_weight, down_weight):
    rows, width = tokens.shape
    heads = forget.shape[1]
    inner = projections.shape[2]
    hidden = down_weight.shape[0]
    pairs = heads // 2
    steps = max(blocks - 1, 0).bit_length()
    chunk = rows // CHUNKS
    half = chunk // 2
    V = pltpu.VMEM
    S = pltpu.SemaphoreType.DMA
    slots = max(steps, 1)
    piece = V((CHUNKS, half, width), BF16)
    scratch = [
        V((rows, width), BF16),
        V((width, inner), BF16), V((width, inner), BF16), V((width, inner), BF16),
        V((inner, width), BF16),
        V((width, hidden), BF16), V((width, hidden), BF16), V((hidden, width), BF16),
        V((rows, width), BF16),
        V((rows, inner), BF16), V((rows, inner), BF16), V((rows, inner), BF16),
        V((rows, inner), F32), V((rows, inner), BF16),
        V((pairs, 128, 128), BF16),
        V((64 * pairs, 128), F32), V((8, 128), F32), V((64 * pairs, 128), F32), V((8, 128), F32),
        V((slots, 64 * pairs, 128), BF16), V((slots, 8, 128), F32),
        V((slots, 64 * pairs, 128), BF16), V((slots, 8, 128), F32),
        V((chunk, width), F32), V((CHUNKS, half, width), F32),
        piece, piece, piece, piece,
        V((rows, width), BF16), piece, V((chunk, hidden), BF16),
        piece, piece, piece, piece, piece,
        V((rows, heads), F32), V((heads, rows), F32),
        S((8,)), S((slots, 2)), S((slots, 2)),
    ] + [S((CHUNKS,)) for _ in range(13)]
    hbm = pl.BlockSpec(memory_space=pl.ANY)
    vmem = pl.BlockSpec(memory_space=pltpu.VMEM)
    return pl.pallas_call(
        functools.partial(kernel, blocks, steps),
        out_shape=jax.ShapeDtypeStruct((rows, width), BF16),
        in_specs=[hbm, vmem, vmem, hbm, hbm, vmem, hbm, hbm],
        out_specs=hbm,
        scratch_shapes=scratch,
        compiler_params=pltpu.CompilerParams(
            collective_id=0, has_side_effects=True, vmem_limit_bytes=64_000_000
        ),
    )(
        tokens, forget.T, attn_gain[None, :], projections, out_weight,
        ffn_gain[None, :], expand_weight, down_weight,
    )


def solution(mesh):
    placed = (
        P("seq", None),
        P("seq", "tp"),
        P(),
        P(None, None, "tp"),
        P("tp", None),
        P(),
        P(None, None, "tp"),
        P("tp", None),
    )
    return jax.shard_map(
        functools.partial(local, mesh.shape["seq"]),
        mesh=mesh, in_specs=placed, out_specs=P("seq", None), check_vma=False,
    )
```

```python
import functools

import jax
import jax.numpy as jnp
from jax import lax
from jax.experimental import pallas as pl
from jax.experimental.pallas import tpu as pltpu
from jax.sharding import PartitionSpec as P

norm_epsilon = 1e-05
head_epsilon = 1e-06
MESH = pl.DeviceIdType.MESH
CHUNKS = 4
F32 = jnp.float32
BF16 = jnp.bfloat16


def dot(a, b):
    return jnp.dot(a, b, preferred_element_type=F32)


def contract(a, b, dim_a, dim_b):
    return lax.dot_general(
        a, b, (((dim_a,), (dim_b,)), ((), ())), preferred_element_type=F32
    )


def normalize(widened, gain):
    mean_square = jnp.mean(widened * widened, axis=-1, keepdims=True)
    return (widened * lax.rsqrt(mean_square + norm_epsilon) * gain).astype(BF16)


def kernel(
    blocks, steps,
    tok, fgt, again, proj_hbm, ow_hbm, fgain, ew_hbm, dw_hbm,
    out,
    wq, wk, wv, wo, wg, wu, wd,
    normed, q, k, v, att, ho, bd, es, el, ts, tl, tsb, tsl, trb, trl,
    part, own, dsend1, drecv1, xsend1, xrecv1, nf, res, hid,
    dsend2, drecv2, xsend2, xrecv2,
    ld, ldt,
    wsem, sts, strv, d1s, d1r, x1s, x1r, ns, nr, d2s, d2r, x2s, x2r, osd, orv,
):
    rows, width = tok.shape
    heads = fgt.shape[0]
    pairs = heads // 2
    chunk = rows // CHUNKS
    half = chunk // 2
    me = lax.axis_index("seq")
    tp = lax.axis_index("tp")
    core = lax.rem(tp, 2)
    partner = tp + 1 - 2 * core
    across = lax.rem(tp + 2, 4)

    loads = []
    for at, (src, dst) in enumerate((
        (proj_hbm.at[1], wk), (proj_hbm.at[2], wv), (proj_hbm.at[0], wq),
        (ow_hbm, wo), (ew_hbm.at[0], wg), (ew_hbm.at[1], wu), (dw_hbm, wd),
    )):
        copy = pltpu.make_async_copy(src, dst, wsem.at[at])
        loads.append(copy)
    for at in range(2):
        loads[at].start()

    barrier = pltpu.get_barrier_semaphore()
    for other in (partner, across):
        pl.semaphore_signal(barrier, inc=1, device_id={"tp": other}, device_id_type=MESH)
    for step in range(steps):
        for far in (2 ** step, blocks - 2 ** step):
            pl.semaphore_signal(
                barrier, inc=1, device_id={"seq": lax.rem(me + far, blocks)}, device_id_type=MESH)

    tri = (
        lax.broadcasted_iota(jnp.int32, (rows, rows), 0)
        >= lax.broadcasted_iota(jnp.int32, (rows, rows), 1)
    ).astype(F32)
    ld[...] = lax.dot_general(
        tri, fgt[...], (((1,), (1,)), ((), ())),
        precision=lax.Precision.HIGHEST, preferred_element_type=F32,
    )
    ldt[...] = lax.dot_general(
        fgt[...], tri, (((1,), (1,)), ((), ())),
        precision=lax.Precision.HIGHEST, preferred_element_type=F32,
    )

    def norm_chunk(r, carry):
        at = pl.ds(pl.multiple_of(r * chunk, chunk), chunk)
        normed[at, :] = normalize(tok[at, :].astype(F32), again[...])
        return carry

    lax.fori_loop(0, CHUNKS, norm_chunk, 0)

    def project(weight, dst):
        tile = min(256, dst.shape[1])

        def body(j, carry):
            at = pl.ds(pl.multiple_of(j * tile, tile), tile)
            dst[:, at] = dot(normed[...], weight[:, at]).astype(BF16)
            return carry

        lax.fori_loop(0, dst.shape[1] // tile, body, 0)

    loads[0].wait()
    for at in (2, 3):
        loads[at].start()
    project(wk, k)
    loads[1].wait()
    project(wv, v)

    low = lax.broadcasted_iota(jnp.int32, (1, 128), 1) < 64
    low_f = low.astype(F32)
    masks_f = (low_f, 1.0 - low_f)
    masks = (masks_f[0].astype(BF16), masks_f[1].astype(BF16))

    def spread(columns, p):
        return jnp.where(low, columns[:, 2 * p : 2 * p + 1], columns[:, 2 * p + 1 : 2 * p + 2])

    log_decay = ld[...]
    last = log_decay[rows - 1 : rows, :]
    shrink = jnp.exp(last - log_decay)
    tl[...] = jnp.zeros_like(tl)
    el[...] = jnp.zeros_like(el)
    es[...] = jnp.zeros_like(es)
    for p in range(pairs):
        lanes = slice(128 * p, 128 * p + 128)
        scaled = (k[:, lanes].astype(F32) * spread(shrink, p)).astype(BF16)
        state = contract(scaled, v[:, lanes], 0, 0)
        ts[64 * p : 64 * p + 64, :] = state[:64] * masks_f[0] + state[64:] * masks_f[1]
        tl[p : p + 1, :] = spread(last, p)

    pl.semaphore_wait(barrier, 2 + 2 * steps)

    def state_copies(step):
        far = 2 ** step
        return (
            pltpu.make_async_remote_copy(
                tsb.at[step], trb.at[step], sts.at[step, 0], strv.at[step, 0],
                device_id={"seq": me + far}, device_id_type=MESH),
            pltpu.make_async_remote_copy(
                tsl.at[step], trl.at[step], sts.at[step, 1], strv.at[step, 1],
                device_id={"seq": me + far}, device_id_type=MESH),
        )

    def send_state(step):
        @pl.when(me + 2 ** step < blocks)
        def _():
            tsb[step] = ts[...].astype(BF16)
            tsl[step] = tl[...]
            for copy in state_copies(step):
                copy.start()

    def take_state(step):
        @pl.when(me >= 2 ** step)
        def _():
            for copy in state_copies(step):
                copy.wait_recv()
            e_decay = jnp.exp(el[...])
            t_decay = jnp.exp(tl[...])
            for p in range(pairs):
                at = slice(64 * p, 64 * p + 64)
                came = trb[step, at, :].astype(F32)
                es[at, :] = es[at, :] + e_decay[p : p + 1, :] * came
                ts[at, :] = ts[at, :] + t_decay[p : p + 1, :] * came
            el[...] = el[...] + trl[step]
            tl[...] = tl[...] + trl[step]

        if step + 1 < steps:
            send_state(step + 1)

    if steps:
        send_state(0)
    for at in (4, 5, 6):
        loads[at].start()
    loads[2].wait()
    project(wq, q)

    span = rows // 2
    taken = 0
    for p in range(pairs):
        lanes = slice(128 * p, 128 * p + 128)
        for piece in range(2):
            at = slice(piece * span, piece * span + span)
            reach = (piece + 1) * span
            causal = (
                lax.broadcasted_iota(jnp.int32, (span, reach), 0) + piece * span
                >= lax.broadcasted_iota(jnp.int32, (span, reach), 1)
            )
            sums = []
            for j in range(2):
                h = 2 * p + j
                scores = contract(q[at, lanes] * masks[j], k[:reach, lanes], 1, 1)
                gaps = jnp.where(causal, ld[at, h : h + 1] - ldt[h : h + 1, :reach], -1e30)
                weights = (scores * 0.125 * jnp.exp(gaps)).astype(BF16)
                sums.append(dot(weights, v[:reach, lanes]))
            att[at, lanes] = jnp.where(low, sums[0], sums[1])
            if 2 * p + piece in (1, pairs) and taken < steps:
                take_state(taken)
                taken += 1
    while taken < steps:
        take_state(taken)
        taken += 1

    for p in range(pairs):
        came = es[64 * p : 64 * p + 64, :]
        bd[p] = jnp.concatenate([came * masks_f[0], came * masks_f[1]], axis=0).astype(BF16)
    same_head = (
        (lax.broadcasted_iota(jnp.int32, (128, 128), 0) < 64)
        == (lax.broadcasted_iota(jnp.int32, (128, 128), 1) < 64)
    ).astype(F32).astype(BF16)

    def whole_rows(r):
        return pl.ds(pl.multiple_of(r * chunk, chunk), chunk)

    def own_rows(r):
        return pl.ds(pl.multiple_of(r * chunk + core * half, half), half)

    mine = pl.ds(pl.multiple_of(core * half, half), half)
    theirs = pl.ds(pl.multiple_of(half - core * half, half), half)

    def to(src, dst, ssem, rsem, other):
        return pltpu.make_async_remote_copy(
            src, dst, ssem, rsem, device_id={"tp": other}, device_id_type=MESH)

    def d1(r):
        return to(dsend1.at[r], drecv1.at[r], d1s.at[r], d1r.at[r], partner)

    def x1(r):
        return to(xsend1.at[r], xrecv1.at[r], x1s.at[r], x1r.at[r], across)

    def nfc(r):
        return to(nf.at[own_rows(r)], nf.at[own_rows(r)], ns.at[r], nr.at[r], partner)

    def d2(r):
        return to(dsend2.at[r], drecv2.at[r], d2s.at[r], d2r.at[r], partner)

    def x2(r):
        return to(xsend2.at[r], xrecv2.at[r], x2s.at[r], x2r.at[r], across)

    def oc(r):
        return to(out.at[own_rows(r)], out.at[own_rows(r)], osd.at[r], orv.at[r], partner)

    loads[3].wait()
    wide = min(512, width)

    def attend(r, carry):
        at = whole_rows(r)
        reach_decay = jnp.exp(ld[at, :]) * 0.125
        for p in range(pairs):
            lanes = slice(128 * p, 128 * p + 128)
            attended = att[at, lanes] + dot(q[at, lanes], bd[p]) * spread(reach_decay, p)
            mean_square = dot((attended * attended).astype(BF16), same_head) * (1.0 / 64)
            ho[at, lanes] = (attended * lax.rsqrt(mean_square + head_epsilon)).astype(BF16)
        for c in range(width // wide):
            cols = slice(c * wide, c * wide + wide)
            part[:, cols] = dot(ho[at, :], wo[:, cols])
        own[r] = part[mine, :]
        dsend1[r] = part[theirs, :].astype(BF16)
        d1(r).start()
        return carry

    def cross1(r):
        d1(r).wait_recv()
        xsend1[r] = (own[r] + drecv1[r].astype(F32)).astype(BF16)
        x1(r).start()

    def attend_cross(r, carry):
        attend(r, 0)

        @pl.when(r > 0)
        def _():
            cross1(r - 1)

        return carry

    lax.fori_loop(0, CHUNKS, attend_cross, 0)
    cross1(CHUNKS - 1)
    for at in (4, 5, 6):
        loads[at].wait()

    hidden_width = wg.shape[1]
    tile = min(256, hidden_width)

    def forward(r, carry):
        x1(r).wait_recv()
        added = xsend1[r].astype(F32) + xrecv1[r].astype(F32)
        kept = (tok[own_rows(r), :].astype(F32) + added).astype(BF16)
        res[r] = kept
        nf[own_rows(r), :] = normalize(kept.astype(F32), fgain[...])
        nfc(r).start()
        nfc(r).wait_recv()
        at = whole_rows(r)
        for c in range(hidden_width // tile):
            cols = slice(c * tile, c * tile + tile)
            gate = dot(nf[at, :], wg[:, cols])
            up = dot(nf[at, :], wu[:, cols])
            hid[:, cols] = (gate / (1.0 + jnp.exp(-gate)) * up).astype(BF16)
        for c in range(width // wide):
            cols = slice(c * wide, c * wide + wide)
            part[:, cols] = dot(hid[...], wd[:, cols])
        own[r] = part[mine, :]
        dsend2[r] = part[theirs, :].astype(BF16)
        d2(r).start()
        d2(r).wait_recv()
        xsend2[r] = (own[r] + drecv2[r].astype(F32)).astype(BF16)
        x2(r).start()
        return carry

    lax.fori_loop(0, CHUNKS, forward, 0)

    def finish(r, carry):
        x2(r).wait_recv()
        added = xsend2[r].astype(F32) + xrecv2[r].astype(F32)
        out[own_rows(r), :] = (res[r].astype(F32) + added).astype(BF16)
        oc(r).start()
        return carry

    lax.fori_loop(0, CHUNKS, finish, 0)

    def drain(r, carry):
        for copy in (d1(r), x1(r), nfc(r), d2(r), x2(r)):
            copy.wait_send()
        oc(r).wait()
        return carry

    lax.fori_loop(0, CHUNKS, drain, 0)
    for step in range(steps):
        @pl.when(me + 2 ** step < blocks)
        def _():
            for copy in state_copies(step):
                copy.wait_send()


def local(blocks, tokens, forget, attn_gain, projections, out_weight, ffn_gain, expand_weight, down_weight):
    rows, width = tokens.shape
    heads = forget.shape[1]
    inner = projections.shape[2]
    hidden = down_weight.shape[0]
    pairs = heads // 2
    steps = max(blocks - 1, 0).bit_length()
    chunk = rows // CHUNKS
    half = chunk // 2
    V = pltpu.VMEM
    S = pltpu.SemaphoreType.DMA
    slots = max(steps, 1)
    piece = V((CHUNKS, half, width), BF16)
    scratch = [
        V((width, inner), BF16), V((width, inner), BF16), V((width, inner), BF16),
        V((inner, width), BF16),
        V((width, hidden), BF16), V((width, hidden), BF16), V((hidden, width), BF16),
        V((rows, width), BF16),
        V((rows, inner), BF16), V((rows, inner), BF16), V((rows, inner), BF16),
        V((rows, inner), F32), V((rows, inner), BF16),
        V((pairs, 128, 128), BF16),
        V((64 * pairs, 128), F32), V((8, 128), F32), V((64 * pairs, 128), F32), V((8, 128), F32),
        V((slots, 64 * pairs, 128), BF16), V((slots, 8, 128), F32),
        V((slots, 64 * pairs, 128), BF16), V((slots, 8, 128), F32),
        V((chunk, width), F32), V((CHUNKS, half, width), F32),
        piece, piece, piece, piece,
        V((rows, width), BF16), piece, V((chunk, hidden), BF16),
        piece, piece, piece, piece,
        V((rows, heads), F32), V((heads, rows), F32),
        S((8,)), S((slots, 2)), S((slots, 2)),
    ] + [S((CHUNKS,)) for _ in range(12)]
    hbm = pl.BlockSpec(memory_space=pl.ANY)
    vmem = pl.BlockSpec(memory_space=pltpu.VMEM)
    return pl.pallas_call(
        functools.partial(kernel, blocks, steps),
        out_shape=jax.ShapeDtypeStruct((rows, width), BF16),
        in_specs=[vmem, vmem, vmem, hbm, hbm, vmem, hbm, hbm],
        out_specs=vmem,
        scratch_shapes=scratch,
        compiler_params=pltpu.CompilerParams(
            collective_id=0, has_side_effects=True, vmem_limit_bytes=52_000_000
        ),
    )(
        tokens, forget.T, attn_gain[None, :], projections, out_weight,
        ffn_gain[None, :], expand_weight, down_weight,
    )


def solution(mesh):
    placed = (
        P("seq", None),
        P("seq", "tp"),
        P(),
        P(None, None, "tp"),
        P("tp", None),
        P(),
        P(None, None, "tp"),
        P("tp", None),
    )
    return jax.shard_map(
        functools.partial(local, mesh.shape["seq"]),
        mesh=mesh, in_specs=placed, out_specs=P("seq", None), check_vma=False,
    )
```
